32 devices in a mesh: dof: 8 (over y, x, core), tm: 4 (over z).
Axes of the slice: x: 2, y: 2, z: 4, core: 2. Of those that a mesh axis runs over, the one named last changes fastest.
Arguments:
- snapshots: bfloat16 [163840, 1024], P('dof', 'tm'), may hold values from -6 to 6
- basis: bfloat16 [163840, 64], P('dof'), may hold values from -0.015625 to 0.015625
Outputs:
- gram: float32 [2144, 2144], P('tm', 'dof')
- coords: float32 [64, 1024], P(None, 'tm')
The draws below stay inside these ranges and needn't reach their ends.
All inputs are finite; a program needn't handle non-finite values.
Results may differ from the reference program's by a relative error of at most 0.0021.
Values may be sent and summed in bfloat16 or wider, within the bound.
No kernel may reach another device: no remote copies, remote signals or barrier semaphores. Data moves between devices by JAX's collectives and lax.ppermute only.
A program may use at most 64 MiB of HBM per device.

```python
import jax
import jax.numpy as jnp
import numpy as np
from jax import lax

R = 64
NDOF = 163840
NT = 1024


def level_of(rng, shape, cuts, least, high):
    factor_of = 1.0
    for axis_at, parts in cuts:
        draws = jax.random.uniform(jax.random.fold_in(jax.random.fold_in(rng, 6), axis_at), (parts,), jnp.float32, least / len(cuts), high / len(cuts))
        factor_of = factor_of * jnp.repeat(jnp.exp(draws), shape[axis_at] // parts).reshape((-1,) + (1,) * (len(shape) - 1 - axis_at))
    return factor_of


def gaussian(key, shape, deviation, reach, pieces=(), held_as=jnp.bfloat16):
    result = jax.random.normal(key, shape, jnp.float32) * deviation
    if len(pieces) > 0:
        result = level_of(key, shape, pieces, -0.22, 0.18) * result
    return jnp.clip(result, min=-reach, max=reach).astype(held_as)


def setup_inputs(seed: int = 0) -> dict:
    keys = jax.random.split(jax.random.key(seed), 3)
    return {
        "snapshots": gaussian(keys[0], (NDOF, NT), 1.0, 6.0, ((0, 8), (1, 4))),
        "basis": gaussian(keys[1], (NDOF, R), NDOF ** -0.5, 0.015625, ((0, 8),)),
    }


def build_features(coords):
    modes = coords.shape[0]
    upper_i, upper_j = np.triu_indices(modes)
    quad = coords[upper_i, :] * coords[upper_j, :]
    return jnp.concatenate([coords, quad], axis=0).astype(jnp.bfloat16)


def reference(snapshots, basis):
    coords = lax.dot_general(basis, snapshots, (((0,), (0,)), ((), ())), preferred_element_type=jnp.float32)
    features = build_features(coords)
    gram = lax.dot_general(features, features, (((1,), (1,)), ((), ())), preferred_element_type=jnp.float32)
    gram = gram * (1.0 / NT)
    return gram, coords
```

```python
import functools

import jax
import jax.numpy as jnp
from jax import lax
from jax.experimental import pallas as pl
from jax.experimental.pallas import tpu as pltpu
from jax.sharding import PartitionSpec as P


TERMS = 3


def parity(index, size):
    total = jnp.zeros_like(index)
    for bit in range((size - 1).bit_length()):
        total = total ^ (index >> bit)
    return total & 1


def exchange(value, dof_flip, tm_flip):
    dof, tm = lax.axis_size("dof"), lax.axis_size("tm")
    flip = dof_flip * tm + tm_flip
    return lax.ppermute(value, ("dof", "tm"), [(i, i ^ flip) for i in range(dof * tm)])


def gather_coords(partial):
    modes, _ = partial.shape
    half = modes // 2
    dof, tm = lax.axis_size("dof"), lax.axis_size("tm")
    mine = parity(lax.axis_index("dof"), dof) ^ parity(lax.axis_index("tm"), tm)
    keep = lax.dynamic_slice_in_dim(partial, mine * half, half, 0)
    send = lax.dynamic_slice_in_dim(partial, (1 - mine) * half, half, 0)
    total = keep + exchange(send, 1, 0)
    flip = 2
    while flip < dof:
        total = total + exchange(total, flip | 1, 0)
        flip *= 2
    blocks = [total]
    flip = 1
    while flip < tm:
        held = blocks[0] if len(blocks) == 1 else jnp.concatenate(blocks, axis=0)
        if flip * 2 < tm:
            steps = ((1, flip), (1, flip * 2), (0, flip * 3))
            flip *= 4
        else:
            steps = ((1, flip),)
            flip *= 2
        blocks = [held] + [exchange(held, *step) for step in steps]
    ours = jnp.concatenate(blocks, axis=0)
    theirs = exchange(ours, 1, 0)
    return ours, theirs, mine


def selectors(start, rows, modes, lanes):
    feature = start + lax.broadcasted_iota(jnp.int32, (rows, lanes), 0)
    lane = lax.broadcasted_iota(jnp.int32, (rows, lanes), 1)
    pair = jnp.maximum(feature - modes, 0)
    odd = 2 * modes + 1
    root = jnp.sqrt((odd * odd - 8 * pair).astype(jnp.float32))
    first = ((odd - root) * 0.5).astype(jnp.int32)

    def begin(i):
        return i * modes - (i * (i - 1)) // 2

    first = jnp.where(begin(first) > pair, first - 1, first)
    first = jnp.where(begin(first + 1) <= pair, first + 1, first)
    second = pair - begin(first) + first
    linear = feature < modes
    first = jnp.where(linear, feature, first)
    in_terms = lane < TERMS * modes
    mode = lane % modes
    pick_first = in_terms & (mode == first)
    pick_second = jnp.where(linear, lane == TERMS * modes, in_terms & (mode == second))
    return pick_first.astype(jnp.bfloat16), pick_second.astype(jnp.bfloat16)


def gram_kernel(scale, mine_ref, ours_ref, theirs_ref, row_a, row_b, col_a, col_b, gram_ref, coords_ref, held, terms):
    half = coords_ref.shape[0] // 2
    modes, width = 2 * half, coords_ref.shape[1]
    blocks = ours_ref.shape[0] // half
    mine = mine_ref[0]
    tail = lax.broadcasted_iota(jnp.int32, (terms.shape[1] - TERMS * modes, width), 0)
    for block in range(blocks):
        rows = pl.ds(block * half, half)
        held[pl.ds(pl.multiple_of(mine * half, half), half), :] = ours_ref[rows, :]
        held[pl.ds(pl.multiple_of((1 - mine) * half, half), half), :] = theirs_ref[rows, :]
        rest = held[...]
        if block == 0:
            coords_ref[...] = rest
        for term in range(TERMS):
            part = rest.astype(jnp.bfloat16)
            terms[block, pl.ds(term * modes, modes), :] = part
            rest = rest - part.astype(jnp.float32)
        terms[block, pl.ds(TERMS * modes, tail.shape[0]), :] = (tail == 0).astype(jnp.bfloat16)
    total = jnp.zeros(gram_ref.shape, jnp.float32)
    for block in range(blocks):
        source = terms[block]

        def features(a, b):
            left = jnp.dot(a[...], source, preferred_element_type=jnp.float32)
            right = jnp.dot(b[...], source, preferred_element_type=jnp.float32)
            return (left * right).astype(jnp.bfloat16)

        total = total + lax.dot_general(
            features(col_a, col_b),
            features(row_a, row_b),
            (((1,), (1,)), ((), ())),
            preferred_element_type=jnp.float32,
        )
    gram_ref[...] = total * scale


def on_device(snapshots, basis):
    partial = lax.dot_general(
        basis, snapshots, (((0,), (0,)), ((), ())), preferred_element_type=jnp.float32
    )
    modes, width = partial.shape
    dof, tm = lax.axis_size("dof"), lax.axis_size("tm")
    count = modes + modes * (modes + 1) // 2
    rows, cols = count // tm, count // dof
    lanes = -(-(TERMS * modes + 1) // 128) * 128
    row_a, row_b = selectors(lax.axis_index("tm") * rows, rows, modes, lanes)
    col_a, col_b = selectors(lax.axis_index("dof") * cols, cols, modes, lanes)
    ours, theirs, mine = gather_coords(partial)
    vmem = pl.BlockSpec(memory_space=pltpu.VMEM)
    gram_t, coords = pl.pallas_call(
        functools.partial(gram_kernel, 1.0 / (width * tm)),
        out_shape=(
            jax.ShapeDtypeStruct((cols, rows), jnp.float32),
            jax.ShapeDtypeStruct((modes, width), jnp.float32),
        ),
        in_specs=[pl.BlockSpec(memory_space=pltpu.SMEM)] + [vmem] * 6,
        out_specs=(vmem, vmem),
        scratch_shapes=[
            pltpu.VMEM((modes, width), jnp.float32),
            pltpu.VMEM((tm, lanes, width), jnp.bfloat16),
        ],
        cost_estimate=pl.CostEstimate(
            flops=2 * rows * cols * width * tm, bytes_accessed=4 * rows * cols, transcendentals=0
        ),
    )(mine.reshape(1), ours, theirs, row_a, row_b, col_a, col_b)
    return gram_t.T, coords


def solution(mesh):
    placed = (P("dof", "tm"), P("dof", None))
    return jax.shard_map(
        on_device,
        mesh=mesh,
        in_specs=placed,
        out_specs=(P("tm", "dof"), P(None, "tm")),
        check_vma=False,
    )
```

```python
import functools

import jax
import jax.numpy as jnp
from jax import lax
from jax.experimental import pallas as pl
from jax.experimental.pallas import tpu as pltpu
from jax.sharding import PartitionSpec as P


LANES = 128
CHUNKS = 10
TERMS = 3


def parity(index, size):
    total = jnp.zeros_like(index)
    for bit in range((size - 1).bit_length()):
        total = total ^ (index >> bit)
    return total & 1


def exchange(value, dof_flip, tm_flip):
    dof, tm = lax.axis_size("dof"), lax.axis_size("tm")
    flip = dof_flip * tm + tm_flip
    return lax.ppermute(value, ("dof", "tm"), [(i, i ^ flip) for i in range(dof * tm)])


def gather_coords(keep, send):
    dof, tm = lax.axis_size("dof"), lax.axis_size("tm")
    total = keep + exchange(send, 1, 0)
    flip = 2
    while flip < dof:
        total = total + exchange(total, flip | 1, 0)
        flip *= 2
    blocks = [total]
    flip = 1
    while flip < tm:
        held = blocks[0] if len(blocks) == 1 else jnp.concatenate(blocks, axis=0)
        if flip * 2 < tm:
            steps = ((1, flip), (1, flip * 2), (0, flip * 3))
            flip *= 4
        else:
            steps = ((1, flip),)
            flip *= 2
        blocks = [held] + [exchange(held, *step) for step in steps]
    ours = jnp.concatenate(blocks, axis=0)
    return ours, exchange(ours, 1, 0)


def selectors(start, modes, first_ref, second_ref):
    rows, lanes = first_ref.shape
    feature = start + lax.broadcasted_iota(jnp.int32, (rows, LANES), 0)
    pair = jnp.maximum(feature - modes, 0)
    odd = 2 * modes + 1
    root = jnp.sqrt((odd * odd - 8 * pair).astype(jnp.float32))
    first = ((odd - root) * 0.5).astype(jnp.int32)

    def begin(i):
        return i * modes - ((i * (i - 1)) >> 1)

    first = jnp.where(begin(first) > pair, first - 1, first)
    first = jnp.where(begin(first + 1) <= pair, first + 1, first)
    second = pair - begin(first) + first
    linear = feature < modes
    first = jnp.where(linear, feature, first)
    second = jnp.where(linear, -1, second)
    for at in range(0, lanes, LANES):
        lane = at + lax.broadcasted_iota(jnp.int32, (rows, LANES), 1)
        mode = jnp.where(lane < TERMS * modes, lax.rem(lane, modes), -2)
        mode = jnp.where(lane == TERMS * modes, -1, mode)
        columns = pl.ds(at, LANES)
        first_ref[:, columns] = (mode == first).astype(jnp.float32).astype(jnp.bfloat16)
        second_ref[:, columns] = (mode == second).astype(jnp.float32).astype(jnp.bfloat16)


def project_kernel(place_ref, basis_ref, snapshots_ref, keep_ref, send_ref, row_a, row_b, col_a, col_b,
                   basis_held, snapshots_held, total, basis_sem, snapshots_sem):
    modes = basis_ref.shape[0]
    half = modes // 2
    chunks = snapshots_held.shape[0]
    depth = snapshots_held.shape[1]
    copies = []
    for chunk in range(chunks):
        rows = pl.ds(chunk * depth, depth)
        copies.append((
            pltpu.make_async_copy(basis_ref.at[:, rows], basis_held.at[chunk], basis_sem.at[chunk]),
            pltpu.make_async_copy(snapshots_ref.at[rows, :], snapshots_held.at[chunk], snapshots_sem.at[chunk]),
        ))
        for copy in copies[-1]:
            copy.start()
    selectors(place_ref[1], modes, row_a, row_b)
    selectors(place_ref[2], modes, col_a, col_b)
    partial = None
    for chunk in range(chunks):
        for copy in copies[chunk]:
            copy.wait()
        term = jnp.dot(basis_held[chunk], snapshots_held[chunk], preferred_element_type=jnp.float32)
        partial = term if partial is None else partial + term
    total[...] = partial
    mine = place_ref[0]
    keep_ref[...] = total[pl.ds(pl.multiple_of(mine * half, half), half), :]
    send_ref[...] = total[pl.ds(pl.multiple_of((1 - mine) * half, half), half), :]


def gram_kernel(scale, place_ref, ours_ref, theirs_ref, row_a, row_b, col_a, col_b, gram_ref, coords_ref, held, terms):
    half = coords_ref.shape[0] // 2
    modes, width = 2 * half, coords_ref.shape[1]
    blocks = ours_ref.shape[0] // half
    mine = place_ref[0]
    tail = lax.broadcasted_iota(jnp.int32, (terms.shape[1] - TERMS * modes, width), 0)
    for block in range(blocks):
        rows = pl.ds(block * half, half)
        held[pl.ds(pl.multiple_of(mine * half, half), half), :] = ours_ref[rows, :]
        held[pl.ds(pl.multiple_of((1 - mine) * half, half), half), :] = theirs_ref[rows, :]
        rest = held[...]
        if block == 0:
            coords_ref[...] = rest
        for term in range(TERMS):
            part = rest.astype(jnp.bfloat16)
            terms[block, pl.ds(term * modes, modes), :] = part
            rest = rest - part.astype(jnp.float32)
        terms[block, pl.ds(TERMS * modes, tail.shape[0]), :] = (tail == 0).astype(jnp.bfloat16)
    total = jnp.zeros(gram_ref.shape, jnp.float32)
    for block in range(blocks):
        source = terms[block]

        def features(a, b):
            left = jnp.dot(a[...], source, preferred_element_type=jnp.float32)
            right = jnp.dot(b[...], source, preferred_element_type=jnp.float32)
            return (left * right).astype(jnp.bfloat16)

        total = total + lax.dot_general(
            features(col_a, col_b),
            features(row_a, row_b),
            (((1,), (1,)), ((), ())),
            preferred_element_type=jnp.float32,
        )
    gram_ref[...] = total * scale


def on_device(snapshots, basis):
    depth, width = snapshots.shape
    modes = basis.shape[1]
    half = modes // 2
    dof, tm = lax.axis_size("dof"), lax.axis_size("tm")
    dof_at, tm_at = lax.axis_index("dof"), lax.axis_index("tm")
    count = modes + modes * (modes + 1) // 2
    rows, cols = count // tm, count // dof
    lanes = -(-(TERMS * modes + 1) // LANES) * LANES
    chunks = CHUNKS
    mine = parity(dof_at, dof) ^ parity(tm_at, tm)
    place = jnp.stack([mine, tm_at * rows, dof_at * cols])
    vmem = pl.BlockSpec(memory_space=pltpu.VMEM)
    smem = pl.BlockSpec(memory_space=pltpu.SMEM)
    away = pl.BlockSpec(memory_space=pl.ANY)
    picks = [jax.ShapeDtypeStruct((n, lanes), jnp.bfloat16) for n in (rows, rows, cols, cols)]
    part = jax.ShapeDtypeStruct((half, width), jnp.float32)
    keep, send, *picked = pl.pallas_call(
        project_kernel,
        out_shape=(part, part, *picks),
        in_specs=[smem, away, away],
        out_specs=(vmem,) * 6,
        scratch_shapes=[
            pltpu.VMEM((chunks, modes, depth // chunks), jnp.bfloat16),
            pltpu.VMEM((chunks, depth // chunks, width), jnp.bfloat16),
            pltpu.VMEM((modes, width), jnp.float32),
            pltpu.SemaphoreType.DMA((chunks,)),
            pltpu.SemaphoreType.DMA((chunks,)),
        ],
        compiler_params=pltpu.CompilerParams(vmem_limit_bytes=52 << 20),
        cost_estimate=pl.CostEstimate(
            flops=2 * modes * depth * width, bytes_accessed=2 * depth * (modes + width), transcendentals=0
        ),
    )(place, basis.T, snapshots)
    ours, theirs = gather_coords(keep, send)
    gram_t, coords = pl.pallas_call(
        functools.partial(gram_kernel, 1.0 / (width * tm)),
        out_shape=(
            jax.ShapeDtypeStruct((cols, rows), jnp.float32),
            jax.ShapeDtypeStruct((modes, width), jnp.float32),
        ),
        in_specs=[smem] + [vmem] * 6,
        out_specs=(vmem, vmem),
        scratch_shapes=[
            pltpu.VMEM((modes, width), jnp.float32),
            pltpu.VMEM((tm, lanes, width), jnp.bfloat16),
        ],
        compiler_params=pltpu.CompilerParams(vmem_limit_bytes=16 << 20),
        cost_estimate=pl.CostEstimate(
            flops=2 * rows * cols * width * tm, bytes_accessed=4 * rows * cols, transcendentals=0
        ),
    )(place, ours, theirs, *picked)
    return gram_t.T, coords


def solution(mesh):
    placed = (P("dof", "tm"), P("dof", None))
    return jax.shard_map(
        on_device,
        mesh=mesh,
        in_specs=placed,
        out_specs=(P("tm", "dof"), P(None, "tm")),
        check_vma=False,
    )
```

```python
import functools

import jax
import jax.numpy as jnp
from jax import lax
from jax.experimental import pallas as pl
from jax.experimental.pallas import tpu as pltpu
from jax.sharding import PartitionSpec as P


LANES = 128
CHUNKS = 10
TERMS = 3


def parity(index, size):
    total = index
    for bit in range(1, (size - 1).bit_length()):
        total = total ^ (index >> bit)
    return total & 1


def half_of():
    dof, tm = lax.axis_size("dof"), lax.axis_size("tm")
    return parity(lax.axis_index("dof"), dof) ^ parity(lax.axis_index("tm"), tm)


def exchange(value, dof_flip, tm_flip):
    dof, tm = lax.axis_size("dof"), lax.axis_size("tm")
    flip = dof_flip * tm + tm_flip
    return lax.ppermute(value, ("dof", "tm"), [(i, i ^ flip) for i in range(dof * tm)])


def gather_coords(keep, send):
    dof, tm = lax.axis_size("dof"), lax.axis_size("tm")
    total = keep + exchange(send, 1, 0)
    flip = 2
    while flip < dof:
        if flip * 2 < dof:
            steps = (flip | 1, (flip * 2) | 1, flip * 3)
            flip *= 4
        else:
            steps = (flip | 1,)
            flip *= 2
        total = sum([exchange(total, step, 0) for step in steps], total)
    ours = total
    flip = tm // 2
    while flip > 1:
        ours = jnp.concatenate([ours, exchange(ours, 1, flip)], axis=0)
        flip //= 2
    later = exchange(ours, 1, flip)
    return ours, exchange(ours, 1, 0), later


def selectors(start, modes, first_ref, second_ref):
    rows, lanes = first_ref.shape
    feature = start + lax.broadcasted_iota(jnp.int32, (rows, LANES), 0)
    pair = jnp.maximum(feature - modes, 0)
    odd = 2 * modes + 1
    root = jnp.sqrt((odd * odd - 8 * pair).astype(jnp.float32))
    first = ((odd - root) * 0.5).astype(jnp.int32)

    def begin(i):
        return i * modes - ((i * (i - 1)) >> 1)

    first = jnp.where(begin(first) > pair, first - 1, first)
    first = jnp.where(begin(first + 1) <= pair, first + 1, first)
    second = pair - begin(first) + first
    linear = feature < modes
    first = jnp.where(linear, feature, first)
    second = jnp.where(linear, -1, second)
    for at in range(0, lanes, LANES):
        lane = at + lax.broadcasted_iota(jnp.int32, (rows, LANES), 1)
        mode = jnp.where(lane < TERMS * modes, lax.rem(lane, modes), -2)
        mode = jnp.where(lane == TERMS * modes, -1, mode)
        columns = pl.ds(at, LANES)
        first_ref[:, columns] = (mode == first).astype(jnp.float32).astype(jnp.bfloat16)
        second_ref[:, columns] = (mode == second).astype(jnp.float32).astype(jnp.bfloat16)


def project_kernel(basis_ref, snapshots_ref, keep_ref, send_ref, row_a, row_b, col_a, col_b,
                   basis_held, snapshots_held, total, basis_sem, snapshots_sem):
    modes = basis_ref.shape[0]
    half = modes // 2
    chunks = snapshots_held.shape[0]
    depth = snapshots_held.shape[1]
    copies = []
    for chunk in range(chunks):
        rows = pl.ds(chunk * depth, depth)
        copies.append((
            pltpu.make_async_copy(basis_ref.at[:, rows], basis_held.at[chunk], basis_sem.at[chunk]),
            pltpu.make_async_copy(snapshots_ref.at[rows, :], snapshots_held.at[chunk], snapshots_sem.at[chunk]),
        ))
        for copy in copies[-1]:
            copy.start()
    selectors(lax.axis_index("tm") * row_a.shape[0], modes, row_a, row_b)
    selectors(lax.axis_index("dof") * col_a.shape[0], modes, col_a, col_b)
    partial = None
    for chunk in range(chunks):
        for copy in copies[chunk]:
            copy.wait()
        term = jnp.dot(basis_held[chunk], snapshots_held[chunk], preferred_element_type=jnp.float32)
        partial = term if partial is None else partial + term
    total[...] = partial
    mine = half_of()
    keep_ref[...] = total[pl.ds(pl.multiple_of(mine * half, half), half), :]
    send_ref[...] = total[pl.ds(pl.multiple_of((1 - mine) * half, half), half), :]


def add_gram(ours_ref, theirs_ref, row_a, row_b, col_a, col_b, held, terms, total):
    modes, width = held.shape
    half = modes // 2
    mine = half_of()
    tail = lax.broadcasted_iota(jnp.int32, (terms.shape[1] - TERMS * modes, width), 0)
    for block in reversed(range(terms.shape[0])):
        rows = pl.ds(block * half, half)
        held[pl.ds(pl.multiple_of(mine * half, half), half), :] = ours_ref[rows, :]
        held[pl.ds(pl.multiple_of((1 - mine) * half, half), half), :] = theirs_ref[rows, :]
        rest = held[...]
        for term in range(TERMS):
            part = rest.astype(jnp.bfloat16)
            terms[block, pl.ds(term * modes, modes), :] = part
            rest = rest - part.astype(jnp.float32)
        terms[block, pl.ds(TERMS * modes, tail.shape[0]), :] = (tail == 0).astype(jnp.bfloat16)
    for block in range(terms.shape[0]):
        source = terms[block]

        def features(a, b):
            left = jnp.dot(a[...], source, preferred_element_type=jnp.float32)
            right = jnp.dot(b[...], source, preferred_element_type=jnp.float32)
            return (left * right).astype(jnp.bfloat16)

        term = lax.dot_general(
            features(col_a, col_b),
            features(row_a, row_b),
            (((1,), (1,)), ((), ())),
            preferred_element_type=jnp.float32,
        )
        total = term if total is None else total + term
    return total


def first_kernel(ours_ref, theirs_ref, row_a, row_b, col_a, col_b, gram_ref, coords_ref, held, terms):
    gram_ref[...] = add_gram(ours_ref, theirs_ref, row_a, row_b, col_a, col_b, held, terms, None)
    coords_ref[...] = held[...]


def last_kernel(scale, ours_ref, theirs_ref, row_a, row_b, col_a, col_b, sum_ref, gram_ref, held, terms):
    total = add_gram(ours_ref, theirs_ref, row_a, row_b, col_a, col_b, held, terms, sum_ref[...])
    gram_ref[...] = total * scale


def on_device(snapshots, basis):
    depth, width = snapshots.shape
    modes = basis.shape[1]
    half = modes // 2
    dof, tm = lax.axis_size("dof"), lax.axis_size("tm")
    count = modes + modes * (modes + 1) // 2
    rows, cols = count // tm, count // dof
    lanes = -(-(TERMS * modes + 1) // LANES) * LANES
    chunks = CHUNKS
    vmem = pl.BlockSpec(memory_space=pltpu.VMEM)
    away = pl.BlockSpec(memory_space=pl.ANY)
    picks = [jax.ShapeDtypeStruct((n, lanes), jnp.bfloat16) for n in (rows, rows, cols, cols)]
    part = jax.ShapeDtypeStruct((half, width), jnp.float32)
    keep, send, *picked = pl.pallas_call(
        project_kernel,
        out_shape=(part, part, *picks),
        in_specs=[away, away],
        out_specs=(vmem,) * 6,
        scratch_shapes=[
            pltpu.VMEM((chunks, modes, depth // chunks), jnp.bfloat16),
            pltpu.VMEM((chunks, depth // chunks, width), jnp.bfloat16),
            pltpu.VMEM((modes, width), jnp.float32),
            pltpu.SemaphoreType.DMA((chunks,)),
            pltpu.SemaphoreType.DMA((chunks,)),
        ],
        compiler_params=pltpu.CompilerParams(vmem_limit_bytes=52 << 20),
        cost_estimate=pl.CostEstimate(
            flops=2 * modes * depth * width, bytes_accessed=2 * depth * (modes + width), transcendentals=0
        ),
    )(basis.T, snapshots)
    ours, theirs, later = gather_coords(keep, send)
    gram = jax.ShapeDtypeStruct((cols, rows), jnp.float32)
    settings = dict(
        scratch_shapes=[
            pltpu.VMEM((modes, width), jnp.float32),
            pltpu.VMEM((tm // 2, lanes, width), jnp.bfloat16),
        ],
        compiler_params=pltpu.CompilerParams(vmem_limit_bytes=16 << 20),
        cost_estimate=pl.CostEstimate(
            flops=rows * cols * width * tm, bytes_accessed=4 * rows * cols, transcendentals=0
        ),
    )
    half_gram, coords = pl.pallas_call(
        first_kernel,
        out_shape=(gram, jax.ShapeDtypeStruct((modes, width), jnp.float32)),
        in_specs=[vmem] * 6,
        out_specs=(vmem, vmem),
        **settings,
    )(ours, theirs, *picked)
    later, half_gram = lax.optimization_barrier((later, half_gram))
    gram_t = pl.pallas_call(
        functools.partial(last_kernel, 1.0 / (width * tm)),
        out_shape=gram,
        in_specs=[vmem] * 7,
        out_specs=vmem,
        **settings,
    )(later, exchange(later, 1, 0), *picked, half_gram)
    return gram_t.T, coords


def solution(mesh):
    placed = (P("dof", "tm"), P("dof", None))
    return jax.shard_map(
        on_device,
        mesh=mesh,
        in_specs=placed,
        out_specs=(P("tm", "dof"), P(None, "tm")),
        check_vma=False,
    )
```
